128 devices in a mesh: groups: 4 (over x, y), seq: 16 (over z), tensor: 2 (over core).
Axes of the slice: x: 2, y: 2, z: 16, core: 2. Of those that a mesh axis runs over, the one named last changes fastest.
The devices are a block of a 8x8x16 slice.
Arguments:
- patches: bfloat16 [24576, 1152], P(('groups', 'seq')), parts along dimension 0, may hold values from -6 to 6
- vis_up: bfloat16 [1152, 4304], P(None, 'tensor'), may hold values from -0.1875 to 0.1875
- vis_down: bfloat16 [4304, 1152], P('tensor'), may hold values from -0.09375 to 0.09375
- merge_weight: bfloat16 [4608, 5120], P('seq', 'tensor'), may hold values from -0.09375 to 0.09375
- text_states: bfloat16 [12288, 5120], P(('groups', 'seq'), 'tensor'), parts along dimension 0, may hold values from -6 to 6
- w_query: bfloat16 [5120, 4096], P('seq', 'tensor'), may hold values from -2.5 to 2.5, as said below
- w_key: bfloat16 [5120, 512], P('seq', 'tensor'), may hold values from -2.5 to 2.5, as said below
- w_value: bfloat16 [5120, 512], P('seq', 'tensor'), may hold values from -0.078125 to 0.078125
- dest_rows: int32 [6144], P(('groups', 'seq')), parts along dimension 0, may hold values from 0 to 3071, as said below
- doc_ids: int32 [12288], P(('groups', 'seq')), parts along dimension 0, may hold values from 0 to 3, never falling along the last dimension, each value on 1 to 1536 neighbouring positions
Outputs:
- attended: bfloat16 [12288, 4096], P(('groups', 'seq'), 'tensor'), parts along dimension 0
The draws below stay inside these ranges and needn't reach their ends.
There are 4 independent parts, one for each index of `groups`. The reference program is written for one: setup_inputs(seed, part) draws one part's arguments, and reference() takes and returns one part's arrays. A program takes and returns all parts, laid end to end along the dimension named above; an argument that names none is the same for every part. Nothing has to cross between parts.
Inputs may be any that keep to these rules, and one draw needn't show every extreme that they name: `dest_rows`: all entries are distinct; each text shard of 192 positions receives exactly 96 of them; at most 12 of the rows of one seq shard go to one text shard, and some pair reaches 12 in every draw. `w_query`: A query projection of order 5120 ** -0.5 per entry. `w_key`: A key projection of order 5120 ** -0.5 per entry.
All inputs are finite; a program needn't handle non-finite values.
Results may differ from the reference program's by a relative error of at most 0.03.
Values may be sent and summed in bfloat16 or wider, within the bound.
A program may use at most 128 MiB of HBM per device.

```python
import math
import jax
import jax.numpy as jnp
import numpy as np
from jax import lax

VD = 1152
VF = 4304
D = 5120
HEADS = 32
KVH = 4
HD = 128
MD = 4608
M_DEV = 96
TXT_DEV = 192
PATCHES = 6144
MERGED = 1536
TEXT = 3072
N_SEQ = 16


def draw_w_query(key, part):
    base = jax.random.truncated_normal(jax.random.fold_in(key, 21), -4.0, 4.0, (D, HEADS * HD), jnp.float32) * D ** (-0.5)
    return base.astype(jnp.bfloat16)


def draw_w_key(key, part):
    base = jax.random.truncated_normal(jax.random.fold_in(key, 23), -4.0, 4.0, (D, KVH * HD), jnp.float32) * D ** (-0.5)
    return base.astype(jnp.bfloat16)


def draw_dest_rows(key, part):
    shards = N_SEQ
    base = M_DEV // shards
    subkeys = jax.random.split(jax.random.fold_in(key, 31), 5)
    picked = jax.random.permutation(subkeys[0], shards)
    extra = jax.random.randint(subkeys[1], (), 0, base)
    shard_index = jnp.arange(shards, dtype=jnp.int32)

    def marked(which):
        return (shard_index == picked[which]).astype(jnp.int32)
    loads = base + base * (marked(0) - marked(1)) + extra * (marked(2) - marked(3))
    shuffle = jax.random.permutation(subkeys[2], shards)
    counts = loads[(shuffle[None, :] - shard_index[:, None]) % shards]
    running = jnp.cumsum(counts, axis=0)
    slot_index = jnp.arange(M_DEV, dtype=jnp.int32)
    source = jnp.sum((running[:, :, None] <= slot_index[None, None, :]).astype(jnp.int32), axis=0)
    places = jax.vmap(lambda sub: jax.random.permutation(sub, TXT_DEV)[:M_DEV])(jax.random.split(subkeys[3], shards))
    flat_source = source.reshape(-1)
    serial = jnp.arange(MERGED, dtype=jnp.int32)
    same_before = (flat_source[None, :] == flat_source[:, None]) & (serial[None, :] < serial[:, None])
    slot_rank = jnp.sum(same_before.astype(jnp.int32), axis=1)
    orders = jax.vmap(lambda sub: jax.random.permutation(sub, M_DEV))(jax.random.split(subkeys[4], shards))
    row_in_source = orders[flat_source, slot_rank]
    target = (shard_index[:, None] * TXT_DEV + places).reshape(-1).astype(jnp.int32)
    return jnp.zeros((MERGED,), jnp.int32).at[flat_source * M_DEV + row_in_source].set(target)


def shard_levels(key, shape, cuts, low, largest):
    def one(axis_at, parts):
        draws = jax.random.uniform(jax.random.fold_in(jax.random.fold_in(key, 6), axis_at), (parts,), jnp.float32, low / len(cuts), largest / len(cuts))
        return jnp.repeat(jnp.exp(draws), shape[axis_at] // parts).reshape((-1,) + (1,) * (len(shape) - axis_at - 1))

    factor_of = one(*cuts[0])
    for cut in cuts[1:]:
        factor_of = factor_of * one(*cut)
    return factor_of


def profile(number_of, total, bound, lean):
    portions = [(1 << 20) // math.isqrt(standing ** lean) + 1 for standing in range(2, number_of + 1)]
    rest, given = total - bound - (number_of - 1), [1] * (number_of - 1)
    while rest > 0:
        candidates = [i for i in range(number_of - 1) if given[i] < bound]
        whole, remaining = sum([portions[i] for i in candidates]), rest
        for i in candidates:
            addition = min(bound - given[i], max(1, remaining * portions[i] // whole), rest)
            given[i] = given[i] + addition
            rest = rest - addition
    return np.array([bound] + given)


def ragged(stream_key, number_of, total, bound, lean):
    if number_of == 2:
        one = jax.random.randint(stream_key, (), max(1, total - bound), min(bound, total - 1) + 1)
        return jnp.stack([one, total - one])
    lengths = jnp.asarray(profile(number_of, total, bound, lean), jnp.int32)
    pairs = (number_of - 1) // 2
    giver, receiver = lengths[1:1 + 2 * pairs:2], lengths[2:2 + 2 * pairs:2]
    margin = jnp.minimum(giver - 1, bound - receiver)
    moved = jax.random.randint(jax.random.fold_in(stream_key, 1), (pairs,), 0, 1 << 20) % (margin + 1)
    lengths = lengths.at[1:1 + 2 * pairs:2].set(giver - moved).at[2:2 + 2 * pairs:2].set(receiver + moved)
    return lengths[jax.random.permutation(jax.random.fold_in(stream_key, 2), number_of)]


def bell_draw(key, shape, deviation, reach, cuts=(), held_as=jnp.bfloat16):
    array = deviation * jax.random.normal(key, shape, jnp.float32)
    if cuts:
        array = array * shard_levels(key, shape, cuts, -0.22, 0.18)
    return jnp.clip(array, -reach, reach).astype(held_as)


def setup_inputs(seed: int = 0, part: int = 0) -> dict:
    streams_of = jax.random.split(jax.random.key(seed), 11)
    part_keys = jax.random.split(jax.random.fold_in(streams_of[10], part), 11)
    return {
        "patches": bell_draw(part_keys[0], (PATCHES, VD), 1.0, 6.0, ((0, 16),)),
        "vis_up": bell_draw(streams_of[1], (VD, VF), VD ** -0.5, 0.1875, ((1, 2),)),
        "vis_down": bell_draw(streams_of[2], (VF, VD), VF ** -0.5, 0.09375, ((0, 2),)),
        "merge_weight": bell_draw(streams_of[3], (MD, D), MD ** -0.5, 0.09375, ((0, 16), (1, 2))),
        "text_states": bell_draw(part_keys[4], (TEXT, D), 1.0, 6.0, ((0, 16), (1, 2))),
        "w_query": draw_w_query(jax.random.fold_in(streams_of[10], 71), part),
        "w_key": draw_w_key(jax.random.fold_in(streams_of[10], 71), part),
        "w_value": bell_draw(streams_of[7], (D, KVH * HD), D ** -0.5, 0.078125, ((0, 16), (1, 2))),
        "dest_rows": draw_dest_rows(jax.random.fold_in(jax.random.fold_in(streams_of[10], part), 71), part),
        "doc_ids": jnp.searchsorted(jnp.cumsum(ragged(part_keys[9], 4, TEXT, TEXT // 2, 0)), jnp.arange(TEXT), side="right").astype(jnp.int32),
    }


epsilon = 1e-06

def layer_norm(values):
    center = lax.optimization_barrier(jnp.mean(values, axis=-1, keepdims=True))
    spread = lax.optimization_barrier(jnp.mean((values - center) ** 2, axis=-1, keepdims=True))
    return (values - center) * lax.rsqrt(spread + epsilon)

def reference(patches, vis_up, vis_down, merge_weight, text_states, w_query, w_key, w_value, dest_rows, doc_ids):
    values = patches.astype(jnp.float32)
    normed = layer_norm(values).astype(jnp.bfloat16)
    activated = jax.nn.gelu(jnp.dot(normed, vis_up, preferred_element_type=jnp.float32), approximate=True).astype(jnp.bfloat16)
    vision_out = values + jnp.dot(activated, vis_down, preferred_element_type=jnp.float32)
    grouped = layer_norm(vision_out.reshape(MERGED, MD)).astype(jnp.bfloat16)
    block_width = MD // N_SEQ

    def block_sum(running, index):
        offset = (index * block_width).astype(jnp.int32)
        columns = lax.dynamic_slice_in_dim(grouped, offset, block_width, 1)
        weight_rows = lax.dynamic_slice_in_dim(merge_weight, offset, block_width, 0)
        partial_value = jnp.dot(columns, weight_rows, preferred_element_type=jnp.float32)
        rounded = lax.optimization_barrier(partial_value.astype(jnp.bfloat16))
        return (running + rounded.astype(jnp.float32), None)
    merged, _ = lax.scan(block_sum, jnp.zeros((MERGED, D), jnp.float32), jnp.arange(N_SEQ, dtype=jnp.int32))
    merged = merged.astype(jnp.bfloat16)
    routed = jnp.zeros((TEXT, D), jnp.bfloat16).at[dest_rows].set(merged)
    mixed = text_states.astype(jnp.float32) + routed.astype(jnp.float32)
    normed_text = (mixed * lax.rsqrt(lax.optimization_barrier(jnp.mean(mixed * mixed, axis=-1, keepdims=True)) + epsilon)).astype(jnp.bfloat16)
    queries = jnp.dot(normed_text, w_query, preferred_element_type=jnp.float32).astype(jnp.bfloat16)
    keys_all = jnp.dot(normed_text, w_key, preferred_element_type=jnp.float32).astype(jnp.bfloat16)
    values_all = jnp.dot(normed_text, w_value, preferred_element_type=jnp.float32).astype(jnp.bfloat16)
    query_heads = queries.reshape(TEXT, HEADS, HD)
    key_heads = keys_all.reshape(TEXT, KVH, HD)
    value_heads = values_all.reshape(TEXT, KVH, HD)
    group_size = HEADS // KVH
    positions = jnp.arange(TEXT, dtype=jnp.int32)
    visible = (positions[None, :] <= positions[:, None]) & (doc_ids[None, :] == doc_ids[:, None])
    score_scale = HD ** (-0.5)

    def per_head(head):
        query_one = lax.dynamic_index_in_dim(query_heads, head, 1, keepdims=False)
        key_one = lax.dynamic_index_in_dim(key_heads, head // group_size, 1, keepdims=False)
        value_one = lax.dynamic_index_in_dim(value_heads, head // group_size, 1, keepdims=False)
        scores = jnp.dot(query_one, key_one.T, preferred_element_type=jnp.float32) * score_scale
        highest = lax.optimization_barrier(jnp.max(jnp.where(visible, scores, -1e+30), axis=-1, keepdims=True))
        raw = jnp.where(visible, jnp.exp(scores - highest), 0.0)
        mass = lax.optimization_barrier(jnp.sum(raw, axis=-1, keepdims=True))
        summed = jnp.dot(raw.astype(jnp.bfloat16), value_one, preferred_element_type=jnp.float32)
        return (summed / mass).astype(jnp.bfloat16)
    heads_out = lax.map(per_head, jnp.arange(HEADS, dtype=jnp.int32))
    return jnp.transpose(heads_out, (1, 0, 2)).reshape(TEXT, HEADS * HD)
```

```python
import functools
import math

import jax
import jax.numpy as jnp
from jax import lax
from jax.experimental import pallas as pl
from jax.experimental.pallas import tpu as pltpu
from jax.sharding import PartitionSpec as P

HD = 128
BLOCK = 4
REACH = 1536
CLIPS = 4
FAR = -(2.0**100)
LOG2E = 1.4426950408889634

epsilon = 1e-06


def layer_norm(values):
    center = jnp.mean(values, axis=-1, keepdims=True)
    spread = jnp.mean((values - center) ** 2, axis=-1, keepdims=True)
    return (values - center) * lax.rsqrt(spread + epsilon)


def everyones(shard, axis):
    count = lax.axis_size(axis)
    return lax.all_to_all(
        jnp.broadcast_to(shard[None], (count, *shard.shape)), axis, 0, 0, tiled=True
    )


def swap_core(x):
    return lax.ppermute(x, "tensor", [(0, 1), (1, 0)])


def block_swaps():
    groups = lax.axis_size("groups")
    wide = math.isqrt(groups)

    def partner(i, j):
        row, col = divmod(i, wide)
        return (row ^ (j >> 1)) * wide + (col ^ (j & 1))

    swaps = [[(i, partner(i, j)) for i in range(groups)] for j in range(BLOCK)]
    index = lax.axis_index("groups")
    quarter = 2 * ((index // wide) % 2) + index % 2
    return swaps, quarter


def attention_kernel(
    reach, kv_local, group, qkv_ref, doc_q_ref, doc_k_ref, out_ref,
    kv_buf, q_buf, top, total, send_sem, recv_sem,
):
    me = lax.axis_index("seq")
    count = lax.axis_size("seq")
    rows = qkv_ref.shape[1]
    MESH = pl.DeviceIdType.MESH

    barrier = pltpu.get_barrier_semaphore()

    @pl.when(me > 0)
    def _():
        pl.semaphore_signal(barrier, inc=1, device_id={"seq": me - 1}, device_id_type=MESH)

    @pl.when(me < count - 1)
    def _():
        pl.semaphore_signal(barrier, inc=1, device_id={"seq": me + 1}, device_id_type=MESH)

    for i in range(2 * kv_local):
        kv_buf[0, :, i * HD : (i + 1) * HD] = qkv_ref[i, :, :HD]

    pl.semaphore_wait(barrier, jnp.minimum(me, 1) + jnp.minimum(count - 1 - me, 1))

    half = kv_local * HD

    def pass_on(slot, part):
        cols = pl.ds(part * half, half)
        return pltpu.make_async_remote_copy(
            src_ref=kv_buf.at[slot, :, cols],
            dst_ref=kv_buf.at[slot + 1, :, cols],
            send_sem=send_sem.at[slot, part],
            recv_sem=recv_sem.at[slot, part],
            device_id={"seq": me + 1},
            device_id_type=MESH,
        )

    @pl.when(me < count - 1)
    def _():
        pass_on(0, 0).start()
        pass_on(0, 1).start()

    doc_q = doc_q_ref[...]
    per = BLOCK
    for h in range(kv_local * group):
        g, i = divmod(h, group)
        spot = pl.ds(i * rows, rows)
        k, j = divmod(h, per)
        q_buf[g, spot, :HD] = qkv_ref[k, :, (1 + j) * HD : (2 + j) * HD]
        q_buf[g, spot, HD:] = doc_q
    chunk = 2 * rows

    def visit(slot, start):
        doc_k = doc_k_ref[pl.ds(pl.multiple_of(start, rows), rows), :]
        ones = jnp.ones((rows, HD), jnp.bfloat16)

        @pl.loop(0, kv_local)
        def _(g):
            at = pl.multiple_of(g * HD, HD)
            keys = jnp.concatenate([kv_buf[slot, :, pl.ds(at, HD)], doc_k], axis=1)
            vals = jnp.concatenate([kv_buf[slot, :, pl.ds(half + at, HD)], ones], axis=1)
            for b in range(group * rows // chunk):
                spot = pl.ds(b * chunk, chunk)
                s = lax.dot_general(
                    q_buf[g, spot, :], keys, (((1,), (1,)), ((), ())),
                    preferred_element_type=jnp.float32,
                )
                first = isinstance(slot, int)
                if first:
                    token = lax.rem(
                        lax.broadcasted_iota(jnp.int32, s.shape, 0), jnp.int32(rows)
                    )
                    other = lax.broadcasted_iota(jnp.int32, s.shape, 1)
                    s = jnp.where(other <= token, s, FAR)
                    high = jnp.max(s, axis=1, keepdims=True)
                    raw = jnp.exp2(s - high).astype(jnp.bfloat16)
                    total[g, spot, :] = jnp.dot(raw, vals, preferred_element_type=jnp.float32)
                    top[g, spot, :] = high
                else:
                    before = top[g, spot, :]
                    high = jnp.maximum(before, jnp.max(s, axis=1, keepdims=True))
                    raw = jnp.exp2(s - high).astype(jnp.bfloat16)
                    total[g, spot, :] = total[g, spot, :] * jnp.exp2(before - high) + jnp.dot(
                        raw, vals, preferred_element_type=jnp.float32
                    )
                    top[g, spot, :] = high

    visit(0, me * rows)

    @pl.loop(1, reach + 1)
    def _(slot):
        @pl.when(slot <= me)
        def _():
            for part in range(2):
                pass_on(slot - 1, part).wait_recv()

                @pl.when((slot < reach) & (me < count - 1))
                def _():
                    pass_on(slot, part).start()

            visit(slot, (me - slot) * rows)

    for h in range(kv_local * group):
        g, i = divmod(h, group)
        spot = pl.ds(i * rows, rows)
        out_ref[:, h * HD : (h + 1) * HD] = (
            total[g, spot, :HD] / total[g, spot, HD:]
        ).astype(out_ref.dtype)

    @pl.loop(0, reach)
    def _(slot):
        @pl.when((slot <= me) & (me < count - 1))
        def _():
            for part in range(2):
                pass_on(slot, part).wait_send()


def attention(qkv, doc_q, doc_k, kv_local, group):
    rows = qkv.shape[1]
    reach = -(-(REACH - 1) // rows)
    vmem = pl.BlockSpec(memory_space=pltpu.VMEM)
    heads = kv_local * group
    keys = (reach + 1) * rows
    return pl.pallas_call(
        functools.partial(attention_kernel, reach, kv_local, group),
        out_shape=jax.ShapeDtypeStruct((rows, heads * HD), jnp.bfloat16),
        in_specs=[vmem] * 3,
        out_specs=vmem,
        scratch_shapes=[
            pltpu.VMEM((reach + 1, rows, 2 * kv_local * HD), jnp.bfloat16),
            pltpu.VMEM((kv_local, group * rows, 2 * HD), jnp.bfloat16),
            pltpu.VMEM((kv_local, group * rows, 1), jnp.float32),
            pltpu.VMEM((kv_local, group * rows, 2 * HD), jnp.float32),
            pltpu.SemaphoreType.DMA((reach, 2)),
            pltpu.SemaphoreType.DMA((reach, 2)),
        ],
        compiler_params=pltpu.CompilerParams(
            collective_id=0, has_side_effects=True, vmem_limit_bytes=48 << 20
        ),
        cost_estimate=pl.CostEstimate(
            flops=4 * rows * keys * heads * HD,
            bytes_accessed=8 * qkv.size,
            transcendentals=rows * keys * heads,
        ),
        name="attend",
    )(qkv, doc_q, doc_k)


def body(
    patches,
    vis_up,
    vis_down,
    merge_weight,
    text_states,
    w_query,
    w_key,
    w_value,
    dest_rows,
    doc_ids,
):
    f32, bf16 = jnp.float32, jnp.bfloat16
    swaps, quarter = block_swaps()
    core = lax.axis_index("tensor")
    seq_index = lax.axis_index("seq")
    seq_size = lax.axis_size("seq")
    text_rows, half_width = text_states.shape
    query_cols, kv_cols = w_query.shape[1], w_key.shape[1]
    kv_local = kv_cols // HD
    group = query_cols // kv_cols

    def in_block(pieces):
        return [pieces[0]] + [lax.ppermute(pieces[j], "groups", swaps[j]) for j in (1, 2, 3)]

    kv_part, q_part = 2 * kv_cols // BLOCK, query_cols // BLOCK
    w_kv = jnp.concatenate([w_key, w_value], axis=1)
    w_mine = jnp.concatenate(
        [
            lax.dynamic_slice_in_dim(w_kv, quarter * kv_part, kv_part, 1),
            lax.dynamic_slice_in_dim(w_query, quarter * q_part, q_part, 1),
        ],
        axis=1,
    )
    weights = lax.all_gather(w_mine, "seq", axis=0, tiled=True)

    ints = everyones(jnp.concatenate([dest_rows, doc_ids]), "seq")
    merged_rows = dest_rows.shape[0]
    dests, docs = ints[:, :merged_rows], ints[:, merged_rows:].reshape(-1)

    values = patches.astype(f32)
    normed = layer_norm(values).astype(bf16)
    activated = jax.nn.gelu(
        jnp.dot(normed, vis_up, preferred_element_type=f32), approximate=True
    ).astype(bf16)
    partial = jnp.dot(activated, vis_down, preferred_element_type=f32).astype(bf16)
    half_rows = patches.shape[0] // 2
    away = swap_core(lax.dynamic_slice_in_dim(partial, (1 - core) * half_rows, half_rows, 0))
    kept = lax.dynamic_slice_in_dim(partial, core * half_rows, half_rows, 0)
    vision_out = (
        lax.dynamic_slice_in_dim(patches, core * half_rows, half_rows, 0).astype(f32)
        + kept.astype(f32)
        + away.astype(f32)
    )
    grouped = layer_norm(vision_out.reshape(half_rows // 4, 4 * vision_out.shape[1])).astype(bf16)
    mine = lax.all_to_all(grouped, "seq", split_axis=1, concat_axis=0, tiled=True)
    other = swap_core(mine)
    columns = jnp.concatenate([mine, other], axis=0)
    half_merged = merged_rows // 2
    first = lax.dynamic_slice_in_dim(dests, core * half_merged, half_merged, 1).reshape(-1)
    second = lax.dynamic_slice_in_dim(dests, (1 - core) * half_merged, half_merged, 1).reshape(-1)
    dest = jnp.concatenate([first, second])
    rank = jnp.sum((dest[None, :] < dest[:, None]).astype(jnp.int32), axis=1)
    total_rows = rank.shape[0]
    order = jnp.arange(total_rows, dtype=jnp.int32)[:, None] == rank[None, :]
    in_order = jnp.dot(order.astype(bf16), columns, preferred_element_type=f32).astype(bf16)
    products = jnp.dot(in_order, merge_weight, preferred_element_type=f32).astype(bf16)
    products, weights = lax.optimization_barrier((products, weights))
    owned = lax.psum_scatter(products, "seq", scatter_dimension=0, tiled=True)

    ranks_here = seq_index * merged_rows + jnp.arange(merged_rows, dtype=jnp.int32)
    landing = (
        jnp.sum(jnp.where(ranks_here[:, None] == rank[None, :], dest[None, :], 0), axis=1)
        - seq_index * text_rows
    )
    placer = (
        jnp.arange(text_rows, dtype=jnp.int32)[:, None] == landing[None, :]
    ).astype(bf16)

    def project(pieces):
        ours = jnp.concatenate(pieces, axis=0)
        theirs = swap_core(ours)
        w_here = lax.dynamic_slice_in_dim(weights, core * half_width, half_width, 0)
        w_there = lax.dynamic_slice_in_dim(weights, (1 - core) * half_width, half_width, 0)
        out = jnp.dot(ours, w_here, preferred_element_type=f32) + jnp.dot(
            theirs, w_there, preferred_element_type=f32
        )
        out = out.astype(bf16).reshape(BLOCK, -1, out.shape[1])
        return in_block([out[j] for j in range(BLOCK)])

    from_text = project(in_block([text_states] * BLOCK))
    from_image = project(in_block([owned] * BLOCK))

    mixed = text_states.astype(f32) + jnp.dot(placer, owned, preferred_element_type=f32)
    squares = jnp.sum(mixed * mixed, axis=1)
    squares = squares + swap_core(squares)
    scale = lax.rsqrt(squares / (2 * half_width) + epsilon)[:, None]
    made = [
        (a.astype(f32) + jnp.dot(placer, b, preferred_element_type=f32)) * scale
        for a, b in zip(from_text, from_image)
    ]
    col = jnp.arange(kv_part + q_part) >= kv_part
    soft = jnp.where(col, HD ** (-0.5) * LOG2E, 1.0)[None, :].astype(f32)
    made = jnp.stack([(m * soft).astype(bf16) for m in made])
    qkv = jnp.stack(
        [lax.dynamic_index_in_dim(made, k ^ quarter, 0, keepdims=False) for k in range(BLOCK)]
    )
    clip = jnp.arange(HD, dtype=jnp.int32)[None, :]
    doc_q = (doc_ids[:, None] == clip).astype(bf16)
    doc_k = jnp.where((docs[:, None] != clip) & (clip < CLIPS), FAR, 0.0).astype(bf16)
    return attention(qkv, doc_q, doc_k, kv_local, group)


def solution(mesh):
    in_specs = (
        P(("groups", "seq"), None),
        P(None, "tensor"),
        P("tensor", None),
        P("seq", "tensor"),
        P(("groups", "seq"), "tensor"),
        P("seq", "tensor"),
        P("seq", "tensor"),
        P("seq", "tensor"),
        P(("groups", "seq")),
        P(("groups", "seq")),
    )
    out_specs = P(("groups", "seq"), "tensor")
    return jax.shard_map(body, mesh=mesh, in_specs=in_specs, out_specs=out_specs, check_vma=False)
```

```python
import functools
import math

import jax
import jax.numpy as jnp
from jax import lax
from jax.experimental import pallas as pl
from jax.experimental.pallas import tpu as pltpu
from jax.sharding import PartitionSpec as P

HD = 128
BLOCK = 4
REACH = 1536
CLIPS = 4
FAR = -(2.0**100)
LOG2E = 1.4426950408889634

epsilon = 1e-06


def layer_norm(values):
    center = jnp.mean(values, axis=-1, keepdims=True)
    spread = jnp.mean((values - center) ** 2, axis=-1, keepdims=True)
    return (values - center) * lax.rsqrt(spread + epsilon)


def everyones(shard, axis):
    count = lax.axis_size(axis)
    return lax.all_to_all(
        jnp.broadcast_to(shard[None], (count, *shard.shape)), axis, 0, 0, tiled=True
    )


def swap_core(x):
    return lax.ppermute(x, "tensor", [(0, 1), (1, 0)])


def block_swaps():
    groups = lax.axis_size("groups")
    wide = math.isqrt(groups)

    def partner(i, j):
        row, col = divmod(i, wide)
        return (row ^ (j >> 1)) * wide + (col ^ (j & 1))

    swaps = [[(i, partner(i, j)) for i in range(groups)] for j in range(BLOCK)]
    index = lax.axis_index("groups")
    quarter = 2 * ((index // wide) % 2) + index % 2
    return swaps, quarter


def attention_kernel(
    reach, kv_local, group, qkv_ref, doc_q_ref, doc_k_ref, out_ref,
    kv_buf, q_buf, top, total, send_sem, recv_sem,
):
    me = lax.axis_index("seq")
    count = lax.axis_size("seq")
    rows = qkv_ref.shape[0]
    width = qkv_ref.shape[1] // BLOCK
    MESH = pl.DeviceIdType.MESH

    barrier = pltpu.get_barrier_semaphore()

    @pl.when(me > 0)
    def _():
        pl.semaphore_signal(barrier, inc=1, device_id={"seq": me - 1}, device_id_type=MESH)

    @pl.when(me < count - 1)
    def _():
        pl.semaphore_signal(barrier, inc=1, device_id={"seq": me + 1}, device_id_type=MESH)

    wide = math.isqrt(lax.axis_size("groups"))
    index = lax.axis_index("groups")
    own_row, own_col = lax.rem(index // wide, 2), lax.rem(index, 2)

    def columns_of(k, at):
        row, col = k // 2, k % 2
        j = 2 * (row + own_row - 2 * row * own_row) + (col + own_col - 2 * col * own_col)
        return qkv_ref[:, pl.ds(pl.multiple_of(j * width + at * HD, HD), HD)]

    for g in range(kv_local):
        kv_buf[0, g, :, :HD] = columns_of(g, 0)
        kv_buf[0, g, :, HD:] = columns_of(kv_local + g, 0)

    pl.semaphore_wait(barrier, jnp.minimum(me, 1) + jnp.minimum(count - 1 - me, 1))

    piece = rows // 2

    def pass_on(slot, g, part):
        spot = pl.ds(part * piece, piece)
        return pltpu.make_async_remote_copy(
            src_ref=kv_buf.at[slot, g, spot, :],
            dst_ref=kv_buf.at[slot + 1, g, spot, :],
            send_sem=send_sem.at[slot, g, part],
            recv_sem=recv_sem.at[slot, g, part],
            device_id={"seq": me + 1},
            device_id_type=MESH,
        )

    @pl.when(me < count - 1)
    def _():
        for g in range(kv_local):
            for part in range(2):
                pass_on(0, g, part).start()

    doc_q = doc_q_ref[...]
    for h in range(kv_local * group):
        g, i = divmod(h, group)
        spot = pl.ds(i * rows, rows)
        k, j = divmod(h, BLOCK)
        q_buf[g, spot, :HD] = columns_of(k, 1 + j)
        q_buf[g, spot, HD:] = doc_q
    chunk = 2 * rows

    def visit(slot, g, start, own):
        doc_k = doc_k_ref[pl.ds(pl.multiple_of(start, rows), rows), :]
        ones = jnp.ones((rows, HD), jnp.bfloat16)
        keys = jnp.concatenate([kv_buf[slot, g, :, :HD], doc_k], axis=1)
        vals = jnp.concatenate([kv_buf[slot, g, :, HD:], ones], axis=1)
        for b in range(group * rows // chunk):
            spot = pl.ds(b * chunk, chunk)
            s = lax.dot_general(
                q_buf[g, spot, :], keys, (((1,), (1,)), ((), ())),
                preferred_element_type=jnp.float32,
            )
            if own:
                token = lax.rem(lax.broadcasted_iota(jnp.int32, s.shape, 0), jnp.int32(rows))
                other = lax.broadcasted_iota(jnp.int32, s.shape, 1)
                s = jnp.where(other <= token, s, FAR)
                high = jnp.max(s, axis=1, keepdims=True)
                raw = jnp.exp2(s - high).astype(jnp.bfloat16)
                total[g, spot, :] = jnp.dot(raw, vals, preferred_element_type=jnp.float32)
            else:
                before = top[g, spot, :]
                high = jnp.maximum(before, jnp.max(s, axis=1, keepdims=True))
                raw = jnp.exp2(s - high).astype(jnp.bfloat16)
                total[g, spot, :] = total[g, spot, :] * jnp.exp2(before - high) + jnp.dot(
                    raw, vals, preferred_element_type=jnp.float32
                )
            top[g, spot, :] = high

    @pl.loop(0, kv_local)
    def _(g):
        visit(0, g, me * rows, True)

    @pl.loop(1, reach + 1)
    def _(slot):
        @pl.when(slot <= me)
        def _():
            @pl.loop(0, kv_local)
            def _(g):
                for part in range(2):
                    pass_on(slot - 1, g, part).wait_recv()

                    @pl.when((slot < reach) & (me < count - 1))
                    def _():
                        pass_on(slot, g, part).start()

                visit(slot, g, (me - slot) * rows, False)

    for h in range(kv_local * group):
        g, i = divmod(h, group)
        spot = pl.ds(i * rows, rows)
        out_ref[:, h * HD : (h + 1) * HD] = (
            total[g, spot, :HD] / total[g, spot, HD:]
        ).astype(out_ref.dtype)

    @pl.loop(0, reach)
    def _(slot):
        @pl.when((slot <= me) & (me < count - 1))
        def _():
            for g in range(kv_local):
                for part in range(2):
                    pass_on(slot, g, part).wait_send()


def attention(qkv, doc_q, doc_k, kv_local, group):
    rows = qkv.shape[0]
    reach = -(-(REACH - 1) // rows)
    vmem = pl.BlockSpec(memory_space=pltpu.VMEM)
    heads = kv_local * group
    keys = (reach + 1) * rows
    return pl.pallas_call(
        functools.partial(attention_kernel, reach, kv_local, group),
        out_shape=jax.ShapeDtypeStruct((rows, heads * HD), jnp.bfloat16),
        in_specs=[vmem] * 3,
        out_specs=vmem,
        scratch_shapes=[
            pltpu.VMEM((reach + 1, kv_local, rows, 2 * HD), jnp.bfloat16),
            pltpu.VMEM((kv_local, group * rows, 2 * HD), jnp.bfloat16),
            pltpu.VMEM((kv_local, group * rows, 1), jnp.float32),
            pltpu.VMEM((kv_local, group * rows, 2 * HD), jnp.float32),
            pltpu.SemaphoreType.DMA((reach, kv_local, 2)),
            pltpu.SemaphoreType.DMA((reach, kv_local, 2)),
        ],
        compiler_params=pltpu.CompilerParams(
            collective_id=0, has_side_effects=True, vmem_limit_bytes=48 << 20
        ),
        cost_estimate=pl.CostEstimate(
            flops=4 * rows * keys * heads * HD,
            bytes_accessed=8 * qkv.size,
            transcendentals=rows * keys * heads,
        ),
        name="attend",
    )(qkv, doc_q, doc_k)


def body(
    patches,
    vis_up,
    vis_down,
    merge_weight,
    text_states,
    w_query,
    w_key,
    w_value,
    dest_rows,
    doc_ids,
):
    f32, bf16 = jnp.float32, jnp.bfloat16
    swaps, quarter = block_swaps()
    core = lax.axis_index("tensor")
    seq_index = lax.axis_index("seq")
    seq_size = lax.axis_size("seq")
    text_rows, half_width = text_states.shape
    query_cols, kv_cols = w_query.shape[1], w_key.shape[1]
    kv_local = kv_cols // HD
    group = query_cols // kv_cols

    def in_block(pieces):
        return [pieces[0]] + [lax.ppermute(pieces[j], "groups", swaps[j]) for j in (1, 2, 3)]

    kv_part, q_part = 2 * kv_cols // BLOCK, query_cols // BLOCK
    w_kv = jnp.concatenate([w_key, w_value], axis=1)
    w_mine = jnp.concatenate(
        [
            lax.dynamic_slice_in_dim(w_kv, quarter * kv_part, kv_part, 1),
            lax.dynamic_slice_in_dim(w_query, quarter * q_part, q_part, 1),
        ],
        axis=1,
    )
    late = HD
    early = kv_part + q_part - late
    weights = lax.all_gather(w_mine[:, :early], "seq", axis=0, tiled=True)

    ints = everyones(jnp.concatenate([dest_rows, doc_ids]), "seq")
    merged_rows = dest_rows.shape[0]
    dests, docs = ints[:, :merged_rows], ints[:, merged_rows:].reshape(-1)

    values = patches.astype(f32)
    normed = layer_norm(values).astype(bf16)
    activated = jax.nn.gelu(
        jnp.dot(normed, vis_up, preferred_element_type=f32), approximate=True
    ).astype(bf16)
    partial = jnp.dot(activated, vis_down, preferred_element_type=f32).astype(bf16)
    half_rows = patches.shape[0] // 2
    away = swap_core(lax.dynamic_slice_in_dim(partial, (1 - core) * half_rows, half_rows, 0))
    kept = lax.dynamic_slice_in_dim(partial, core * half_rows, half_rows, 0)
    vision_out = (
        lax.dynamic_slice_in_dim(patches, core * half_rows, half_rows, 0).astype(f32)
        + kept.astype(f32)
        + away.astype(f32)
    )
    grouped = layer_norm(vision_out.reshape(half_rows // 4, 4 * vision_out.shape[1])).astype(bf16)
    mine = lax.all_to_all(grouped, "seq", split_axis=1, concat_axis=0, tiled=True)
    other = swap_core(mine)
    columns = jnp.concatenate([mine, other], axis=0)
    half_merged = merged_rows // 2
    first = lax.dynamic_slice_in_dim(dests, core * half_merged, half_merged, 1).reshape(-1)
    second = lax.dynamic_slice_in_dim(dests, (1 - core) * half_merged, half_merged, 1).reshape(-1)
    dest = jnp.concatenate([first, second])
    rank = jnp.sum((dest[None, :] < dest[:, None]).astype(jnp.int32), axis=1)
    total_rows = rank.shape[0]
    order = jnp.arange(total_rows, dtype=jnp.int32)[:, None] == rank[None, :]
    in_order = jnp.dot(order.astype(bf16), columns, preferred_element_type=f32).astype(bf16)
    products = jnp.dot(in_order, merge_weight, preferred_element_type=f32).astype(bf16)
    products, weights = lax.optimization_barrier((products, weights))
    owned = lax.psum_scatter(products, "seq", scatter_dimension=0, tiled=True)

    ranks_here = seq_index * merged_rows + jnp.arange(merged_rows, dtype=jnp.int32)
    landing = (
        jnp.sum(jnp.where(ranks_here[:, None] == rank[None, :], dest[None, :], 0), axis=1)
        - seq_index * text_rows
    )
    placer = (
        jnp.arange(text_rows, dtype=jnp.int32)[:, None] == landing[None, :]
    ).astype(bf16)

    def both_halves(pieces):
        ours = jnp.concatenate(pieces, axis=0)
        return ours, swap_core(ours)

    def project(rows, w):
        ours, theirs = rows
        w_here = lax.dynamic_slice_in_dim(w, core * half_width, half_width, 0)
        w_there = lax.dynamic_slice_in_dim(w, (1 - core) * half_width, half_width, 0)
        out = jnp.dot(ours, w_here, preferred_element_type=f32) + jnp.dot(
            theirs, w_there, preferred_element_type=f32
        )
        return out.astype(bf16).reshape(BLOCK, -1, out.shape[1])

    text_in = both_halves(in_block([text_states] * BLOCK))
    text_out = project(text_in, weights)
    text_out = in_block([text_out[j] for j in range(BLOCK)])
    owned, text_out = lax.optimization_barrier((owned, text_out))
    w_late, owned = lax.optimization_barrier((w_mine[:, early:], owned))
    weights_late = lax.all_gather(w_late, "seq", axis=0, tiled=True)
    image_in = both_halves(in_block([owned] * BLOCK))
    image_out = project(image_in, weights)
    image_late = project(image_in, weights_late)
    text_late = project(text_in, weights_late)
    cut = text_rows // 2
    back = jnp.concatenate(
        [image_out, image_late, text_late[:, :cut], text_late[:, cut:]], axis=2
    )
    back = in_block([back[j] for j in range(BLOCK)])

    mixed = text_states.astype(f32) + jnp.dot(placer, owned, preferred_element_type=f32)
    squares = jnp.sum(mixed * mixed, axis=1)
    squares = squares + swap_core(squares)
    scale = lax.rsqrt(squares / (2 * half_width) + epsilon)[:, None]
    width = early + late
    from_image = jnp.concatenate([p[:, :width] for p in back], axis=1)
    from_text = jnp.concatenate(
        [
            x
            for t, p in zip(text_out, back)
            for x in (
                t,
                jnp.concatenate([p[:, width : width + late], p[:, width + late :]], axis=0),
            )
        ],
        axis=1,
    )
    is_query = jnp.arange(BLOCK * width) % width >= kv_part
    soft = jnp.where(is_query, HD ** (-0.5) * LOG2E, 1.0)[None, :].astype(f32)
    qkv = (
        (from_text.astype(f32) + jnp.dot(placer, from_image, preferred_element_type=f32))
        * scale
        * soft
    ).astype(bf16)
    clip = jnp.arange(HD, dtype=jnp.int32)[None, :]
    doc_q = (doc_ids[:, None] == clip).astype(bf16)
    doc_k = jnp.where((docs[:, None] != clip) & (clip < CLIPS), FAR, 0.0).astype(bf16)
    return attention(qkv, doc_q, doc_k, kv_local, group)


def solution(mesh):
    in_specs = (
        P(("groups", "seq"), None),
        P(None, "tensor"),
        P("tensor", None),
        P("seq", "tensor"),
        P(("groups", "seq"), "tensor"),
        P("seq", "tensor"),
        P("seq", "tensor"),
        P("seq", "tensor"),
        P(("groups", "seq")),
        P(("groups", "seq")),
    )
    out_specs = P(("groups", "seq"), "tensor")
    return jax.shard_map(body, mesh=mesh, in_specs=in_specs, out_specs=out_specs, check_vma=False)
```

```python
import functools
import math

import jax
import jax.numpy as jnp
from jax import lax
from jax.experimental import pallas as pl
from jax.experimental.pallas import tpu as pltpu
from jax.sharding import PartitionSpec as P

HD = 128
BLOCK = 4
REACH = 1536
CLIPS = 4
FAR = -(2.0**100)
LOG2E = 1.4426950408889634

epsilon = 1e-06


def layer_norm(values):
    center = jnp.mean(values, axis=-1, keepdims=True)
    spread = jnp.mean((values - center) ** 2, axis=-1, keepdims=True)
    return (values - center) * lax.rsqrt(spread + epsilon)


def everyones(shard, axis):
    count = lax.axis_size(axis)
    return lax.all_to_all(
        jnp.broadcast_to(shard[None], (count, *shard.shape)), axis, 0, 0, tiled=True
    )


def swap_core(x):
    return lax.ppermute(x, "tensor", [(0, 1), (1, 0)])


def block_swaps():
    groups = lax.axis_size("groups")
    wide = math.isqrt(groups)

    def partner(i, j):
        row, col = divmod(i, wide)
        return (row ^ (j >> 1)) * wide + (col ^ (j & 1))

    swaps = [[(i, partner(i, j)) for i in range(groups)] for j in range(BLOCK)]
    index = lax.axis_index("groups")
    quarter = 2 * ((index // wide) % 2) + index % 2
    return swaps, quarter


def attention_kernel(
    reach, kv_local, group, qkv_ref, doc_q_ref, doc_k_ref, out_ref,
    kv_buf, q_buf, top, total, send_sem, recv_sem,
):
    me = lax.axis_index("seq")
    count = lax.axis_size("seq")
    rows = qkv_ref.shape[0]
    width = qkv_ref.shape[1] // BLOCK
    MESH = pl.DeviceIdType.MESH

    barrier = pltpu.get_barrier_semaphore()

    @pl.when(me > 0)
    def _():
        pl.semaphore_signal(barrier, inc=1, device_id={"seq": me - 1}, device_id_type=MESH)

    @pl.when(me < count - 1)
    def _():
        pl.semaphore_signal(barrier, inc=1, device_id={"seq": me + 1}, device_id_type=MESH)

    wide = math.isqrt(lax.axis_size("groups"))
    index = lax.axis_index("groups")
    own_row, own_col = lax.rem(index // wide, 2), lax.rem(index, 2)

    def columns_of(k, at):
        row, col = k // 2, k % 2
        j = 2 * (row + own_row - 2 * row * own_row) + (col + own_col - 2 * col * own_col)
        return qkv_ref[:, pl.ds(pl.multiple_of(j * width + at * HD, HD), HD)]

    for g in range(kv_local):
        kv_buf[0, g, :, :HD] = columns_of(g, 0)
        kv_buf[0, g, :, HD:] = columns_of(kv_local + g, 0)

    pl.semaphore_wait(barrier, jnp.minimum(me, 1) + jnp.minimum(count - 1 - me, 1))

    piece = rows // 2

    def pass_on(slot, g, part):
        spot = pl.ds(part * piece, piece)
        return pltpu.make_async_remote_copy(
            src_ref=kv_buf.at[slot, g, spot, :],
            dst_ref=kv_buf.at[slot + 1, g, spot, :],
            send_sem=send_sem.at[slot, g, part],
            recv_sem=recv_sem.at[slot, g, part],
            device_id={"seq": me + 1},
            device_id_type=MESH,
        )

    @pl.when(me < count - 1)
    def _():
        for g in range(kv_local):
            for part in range(2):
                pass_on(0, g, part).start()

    doc_q = doc_q_ref[...]
    for h in range(kv_local * group):
        g, i = divmod(h, group)
        spot = pl.ds(i * rows, rows)
        k, j = divmod(h, BLOCK)
        q_buf[g, spot, :HD] = columns_of(k, 1 + j)
        q_buf[g, spot, HD:] = doc_q
    chunk = 2 * rows

    def visit(slot, g, start, own):
        doc_k = doc_k_ref[pl.ds(pl.multiple_of(start, rows), rows), :]
        ones = jnp.ones((rows, HD), jnp.bfloat16)
        keys = jnp.concatenate([kv_buf[slot, g, :, :HD], doc_k], axis=1)
        vals = jnp.concatenate([kv_buf[slot, g, :, HD:], ones], axis=1)
        for b in range(group * rows // chunk):
            spot = pl.ds(b * chunk, chunk)
            s = lax.dot_general(
                q_buf[g, spot, :], keys, (((1,), (1,)), ((), ())),
                preferred_element_type=jnp.float32,
            )
            if own:
                token = lax.rem(lax.broadcasted_iota(jnp.int32, s.shape, 0), jnp.int32(rows))
                other = lax.broadcasted_iota(jnp.int32, s.shape, 1)
                s = jnp.where(other <= token, s, FAR)
                high = jnp.max(s, axis=1, keepdims=True)
                raw = jnp.exp2(s - high).astype(jnp.bfloat16)
                total[g, spot, :] = jnp.dot(raw, vals, preferred_element_type=jnp.float32)
            else:
                before = top[g, spot, :]
                high = jnp.maximum(before, jnp.max(s, axis=1, keepdims=True))
                raw = jnp.exp2(s - high).astype(jnp.bfloat16)
                total[g, spot, :] = total[g, spot, :] * jnp.exp2(before - high) + jnp.dot(
                    raw, vals, preferred_element_type=jnp.float32
                )
            top[g, spot, :] = high

    @pl.loop(0, kv_local)
    def _(g):
        visit(0, g, me * rows, True)

    @pl.loop(1, reach + 1)
    def _(slot):
        @pl.when(slot <= me)
        def _():
            @pl.loop(0, kv_local)
            def _(g):
                for part in range(2):
                    pass_on(slot - 1, g, part).wait_recv()

                    @pl.when((slot < reach) & (me < count - 1))
                    def _():
                        pass_on(slot, g, part).start()

                visit(slot, g, (me - slot) * rows, False)

    for h in range(kv_local * group):
        g, i = divmod(h, group)
        spot = pl.ds(i * rows, rows)
        out_ref[:, h * HD : (h + 1) * HD] = (
            total[g, spot, :HD] / total[g, spot, HD:]
        ).astype(out_ref.dtype)

    @pl.loop(0, reach)
    def _(slot):
        @pl.when((slot <= me) & (me < count - 1))
        def _():
            for g in range(kv_local):
                for part in range(2):
                    pass_on(slot, g, part).wait_send()


def attention(qkv, doc_q, doc_k, kv_local, group):
    rows = qkv.shape[0]
    reach = -(-(REACH - 1) // rows)
    vmem = pl.BlockSpec(memory_space=pltpu.VMEM)
    heads = kv_local * group
    keys = (reach + 1) * rows
    return pl.pallas_call(
        functools.partial(attention_kernel, reach, kv_local, group),
        out_shape=jax.ShapeDtypeStruct((rows, heads * HD), jnp.bfloat16),
        in_specs=[vmem] * 3,
        out_specs=vmem,
        scratch_shapes=[
            pltpu.VMEM((reach + 1, kv_local, rows, 2 * HD), jnp.bfloat16),
            pltpu.VMEM((kv_local, group * rows, 2 * HD), jnp.bfloat16),
            pltpu.VMEM((kv_local, group * rows, 1), jnp.float32),
            pltpu.VMEM((kv_local, group * rows, 2 * HD), jnp.float32),
            pltpu.SemaphoreType.DMA((reach, kv_local, 2)),
            pltpu.SemaphoreType.DMA((reach, kv_local, 2)),
        ],
        compiler_params=pltpu.CompilerParams(
            collective_id=0, has_side_effects=True, vmem_limit_bytes=48 << 20
        ),
        cost_estimate=pl.CostEstimate(
            flops=4 * rows * keys * heads * HD,
            bytes_accessed=8 * qkv.size,
            transcendentals=rows * keys * heads,
        ),
        name="attend",
    )(qkv, doc_q, doc_k)


def body(
    patches,
    vis_up,
    vis_down,
    merge_weight,
    text_states,
    w_query,
    w_key,
    w_value,
    dest_rows,
    doc_ids,
):
    f32, bf16 = jnp.float32, jnp.bfloat16
    swaps, quarter = block_swaps()
    core = lax.axis_index("tensor")
    seq_index = lax.axis_index("seq")
    seq_size = lax.axis_size("seq")
    text_rows, half_width = text_states.shape
    query_cols, kv_cols = w_query.shape[1], w_key.shape[1]
    kv_local = kv_cols // HD
    group = query_cols // kv_cols

    def in_block(pieces):
        return [pieces[0]] + [lax.ppermute(pieces[j], "groups", swaps[j]) for j in (1, 2, 3)]

    kv_part, q_part = 2 * kv_cols // BLOCK, query_cols // BLOCK
    w_kv = jnp.concatenate([w_key, w_value], axis=1)
    w_mine = jnp.concatenate(
        [
            lax.dynamic_slice_in_dim(w_kv, quarter * kv_part, kv_part, 1),
            lax.dynamic_slice_in_dim(w_query, quarter * q_part, q_part, 1),
        ],
        axis=1,
    )
    width = kv_part + q_part
    weights = lax.all_gather(w_mine, "seq", axis=0, tiled=True)

    ints = everyones(jnp.concatenate([dest_rows, doc_ids]), "seq")
    merged_rows = dest_rows.shape[0]
    dests, docs = ints[:, :merged_rows], ints[:, merged_rows:].reshape(-1)

    values = patches.astype(f32)
    normed = layer_norm(values).astype(bf16)
    activated = jax.nn.gelu(
        jnp.dot(normed, vis_up, preferred_element_type=f32), approximate=True
    ).astype(bf16)
    partial = jnp.dot(activated, vis_down, preferred_element_type=f32).astype(bf16)
    half_rows = patches.shape[0] // 2
    away = swap_core(lax.dynamic_slice_in_dim(partial, (1 - core) * half_rows, half_rows, 0))
    kept = lax.dynamic_slice_in_dim(partial, core * half_rows, half_rows, 0)
    vision_out = (
        lax.dynamic_slice_in_dim(patches, core * half_rows, half_rows, 0).astype(f32)
        + kept.astype(f32)
        + away.astype(f32)
    )
    grouped = layer_norm(vision_out.reshape(half_rows // 4, 4 * vision_out.shape[1])).astype(bf16)
    mine = lax.all_to_all(grouped, "seq", split_axis=1, concat_axis=0, tiled=True)
    other = swap_core(mine)
    columns = jnp.concatenate([mine, other], axis=0)
    half_merged = merged_rows // 2
    first = lax.dynamic_slice_in_dim(dests, core * half_merged, half_merged, 1).reshape(-1)
    second = lax.dynamic_slice_in_dim(dests, (1 - core) * half_merged, half_merged, 1).reshape(-1)
    dest = jnp.concatenate([first, second])
    rank = jnp.sum((dest[None, :] < dest[:, None]).astype(jnp.int32), axis=1)
    total_rows = rank.shape[0]
    order = jnp.arange(total_rows, dtype=jnp.int32)[:, None] == rank[None, :]
    in_order = jnp.dot(order.astype(bf16), columns, preferred_element_type=f32).astype(bf16)
    products = jnp.dot(in_order, merge_weight, preferred_element_type=f32).astype(bf16)
    products, weights = lax.optimization_barrier((products, weights))
    owned = lax.psum_scatter(products, "seq", scatter_dimension=0, tiled=True)

    ranks_here = seq_index * merged_rows + jnp.arange(merged_rows, dtype=jnp.int32)
    landing = (
        jnp.sum(jnp.where(ranks_here[:, None] == rank[None, :], dest[None, :], 0), axis=1)
        - seq_index * text_rows
    )
    placer = (
        jnp.arange(text_rows, dtype=jnp.int32)[:, None] == landing[None, :]
    ).astype(bf16)

    def both_halves(pieces):
        ours = jnp.concatenate(pieces, axis=0)
        return ours, swap_core(ours)

    def project(rows, w):
        ours, theirs = rows
        w_here = lax.dynamic_slice_in_dim(w, core * half_width, half_width, 0)
        w_there = lax.dynamic_slice_in_dim(w, (1 - core) * half_width, half_width, 0)
        out = jnp.dot(ours, w_here, preferred_element_type=f32) + jnp.dot(
            theirs, w_there, preferred_element_type=f32
        )
        return out.astype(bf16).reshape(BLOCK, -1, out.shape[1])

    text_out = project(both_halves(in_block([text_states] * BLOCK)), weights)
    text_out = in_block([text_out[j] for j in range(BLOCK)])
    owned, text_out = lax.optimization_barrier((owned, text_out))
    image_out = project(both_halves(in_block([owned] * BLOCK)), weights)
    image_out = in_block([image_out[j] for j in range(BLOCK)])

    mixed = text_states.astype(f32) + jnp.dot(placer, owned, preferred_element_type=f32)
    squares = jnp.sum(mixed * mixed, axis=1)
    squares = squares + swap_core(squares)
    scale = lax.rsqrt(squares / (2 * half_width) + epsilon)[:, None]
    from_image = jnp.concatenate(image_out, axis=1)
    from_text = jnp.concatenate(text_out, axis=1)
    is_query = jnp.arange(BLOCK * width) % width >= kv_part
    soft = jnp.where(is_query, HD ** (-0.5) * LOG2E, 1.0)[None, :].astype(f32)
    qkv = (
        (from_text.astype(f32) + jnp.dot(placer, from_image, preferred_element_type=f32))
        * scale
        * soft
    ).astype(bf16)
    clip = jnp.arange(HD, dtype=jnp.int32)[None, :]
    doc_q = (doc_ids[:, None] == clip).astype(bf16)
    doc_k = jnp.where((docs[:, None] != clip) & (clip < CLIPS), FAR, 0.0).astype(bf16)
    return attention(qkv, doc_q, doc_k, kv_local, group)


def solution(mesh):
    in_specs = (
        P(("groups", "seq"), None),
        P(None, "tensor"),
        P("tensor", None),
        P("seq", "tensor"),
        P(("groups", "seq"), "tensor"),
        P("seq", "tensor"),
        P("seq", "tensor"),
        P("seq", "tensor"),
        P(("groups", "seq")),
        P(("groups", "seq")),
    )
    out_specs = P(("groups", "seq"), "tensor")
    return jax.shard_map(body, mesh=mesh, in_specs=in_specs, out_specs=out_specs, check_vma=False)
```
